128 devices in a mesh: wide: 8 (over z, core), blk: 16 (over y, x).
Axes of the slice: x: 4, y: 4, z: 4, core: 2. Of those that a mesh axis runs over, the one named last changes fastest.
Arguments:
- rhs: float32 [524288, 256], P(('wide', 'blk'))
- near_blocks: bfloat16 [524288, 1536], P(('wide', 'blk')), may hold values from -0.078125 to 0.078125
- source_basis: bfloat16 [524288, 64], P(('wide', 'blk')), may hold values from -0.5 to 0.5
- target_basis: bfloat16 [524288, 64], P(('wide', 'blk')), may hold values from -0.375 to 0.375
- far_coupling: bfloat16 [4096, 4, 64, 64], P(('wide', 'blk')), may hold values from -0.375 to 0.375
- send_ids: int32 [128, 128, 1], P(('wide', 'blk')), may hold values from 0 to 31
- far_list: int32 [128, 128], P(('wide', 'blk')), may hold values from 0 to 127, each once within a row
Outputs:
- solution: float32 [524288, 256], P(('wide', 'blk'))
- residual: float32 [524288, 256], P(('wide', 'blk'))
The draws below stay inside these ranges and needn't reach their ends.
Inputs may be any that keep to these rules, and one draw needn't show every extreme that they name: Each row of far_list names each received slot 0 to 127 exactly once.
All inputs are finite; a program needn't handle non-finite values.
Results may differ from the reference program's by a relative error of at most 0.0035.
The reference program's roundings to bfloat16 on the way (of `vb`, `coef` and `trans`) count: a program that leaves them out, or rounds other values in their place, can miss the bound.
Values may be sent and summed in bfloat16 or wider, within the bound.
No kernel may reach another device: no remote copies, remote signals or barrier semaphores. Data moves between devices by JAX's collectives and lax.ppermute only.
A program may use at most 128 MiB of HBM per device.

```python
import jax
import jax.numpy as jnp
from jax import lax

ROWS = 4096
NRHS = 256
NEAR = 1024
HALO = 256
LEAF = 128
RANK = 64
SLOT = 1
ITERS = 2
LD = 32
FAN = 4
TOTAL = 524288
LEAVES = 4096
N_WIDE = 8
N_BLK = 16
DEVICES = 128


def draw_rhs(key, part):
    total = DEVICES * ROWS
    owner = (jnp.arange(total, dtype=jnp.int32) // ROWS).astype(jnp.float32)
    rising = jnp.exp(jnp.log(3.0) * owner / max(DEVICES - 1, 1))[:, None]
    values = jax.random.normal(jax.random.fold_in(key, 7), (total, NRHS), jnp.float32) * rising
    return jnp.clip(values, -12.0, 12.0)


def set_ends(result, rng, smallest, high):
    extent = result.shape
    place = [jax.random.randint(jax.random.fold_in(rng, axis), (), 0, extent[axis]) for axis in range(len(extent))]
    result = result.at[tuple(place)].set(smallest)
    longest = extent.index(max(extent))
    place[longest] = (place[longest] + 1) % extent[longest]
    return result.at[tuple(place)].set(high)


def level_of(stream_key, extent, shards, least, high):
    def one(dim, shards_of):
        heights = jax.random.uniform(jax.random.fold_in(jax.random.fold_in(stream_key, 6), dim), (shards_of,), jnp.float32, least / len(shards), high / len(shards))
        return jnp.repeat(jnp.exp(heights), extent[dim] // shards_of).reshape((-1,) + (1,) * (len(extent) - dim - 1))

    gain = one(*shards[0])
    for cut in shards[1:]:
        gain = gain * one(*cut)
    return gain


def noise(rng, dims, scale, reach, cuts=(), kind=jnp.bfloat16):
    factor_of = level_of(rng, dims, cuts, -0.22, 0.18) if cuts else 1.0
    array = jax.random.normal(rng, dims, jnp.float32) * scale * factor_of
    return jnp.minimum(jnp.maximum(array, -reach), reach).astype(kind)


def setup_inputs(seed: int = 0) -> dict:
    keys = jax.random.split(jax.random.key(seed), 8)
    return {
        "rhs": draw_rhs(jax.random.fold_in(keys[7], 71), 0),
        "near_blocks": noise(keys[1], (TOTAL, NEAR + 2 * HALO), (4 * (NEAR + 2 * HALO)) ** -0.5, 0.078125, ((0, 128),)),
        "source_basis": noise(keys[2], (TOTAL, RANK), LEAF ** -0.5, 0.5, ((0, 128),)),
        "target_basis": noise(keys[3], (TOTAL, RANK), (4 * RANK) ** -0.5, 0.375, ((0, 128),)),
        "far_coupling": noise(keys[4], (LEAVES, FAN, RANK, RANK), (FAN * RANK) ** -0.5, 0.375, ((0, 128),)),
        "send_ids": set_ends(jax.random.randint(keys[5], (DEVICES, DEVICES, SLOT), 0, LD), jax.random.fold_in(keys[5], 1), 0, LD - 1).astype(jnp.int32),
        "far_list": jax.vmap(lambda own: jax.random.permutation(own, DEVICES * SLOT))(jax.random.split(keys[6], DEVICES)).reshape((DEVICES, LD * FAN)).astype(jnp.int32),
    }


def near_apply(near_rows, ext):
    outs = []
    for j in range(ROWS // NEAR):
        outs.append(jnp.dot(near_rows[j * NEAR:(j + 1) * NEAR].astype(jnp.float32), ext[j * NEAR:j * NEAR + NEAR + 2 * HALO].astype(jnp.float32), preferred_element_type=jnp.float32))
    return jnp.concatenate(outs, axis=0)

def reference(rhs, near_blocks, source_basis, target_basis, far_coupling, send_ids, far_list):
    fanout = far_list.shape[1] // LD

    def apply(resid):
        vb = resid.astype(jnp.bfloat16)
        grid = vb.reshape(N_WIDE, N_BLK, ROWS, NRHS)
        ext_all = jnp.concatenate([jnp.roll(grid, 1, axis=1)[:, :, ROWS - HALO:], grid, jnp.roll(grid, -1, axis=1)[:, :, :HALO]], axis=2)
        ext_all = ext_all.reshape(DEVICES, ROWS + 2 * HALO, NRHS)
        basis = source_basis.astype(jnp.float32).reshape(DEVICES * LD, LEAF, RANK)
        coef = jnp.einsum('lia,lis->las', basis, vb.astype(jnp.float32).reshape(DEVICES * LD, LEAF, NRHS))
        coef = coef.astype(jnp.bfloat16).reshape(DEVICES, LD, RANK, NRHS)
        sources = jnp.arange(DEVICES, dtype=jnp.int32)[:, None]

        def one_device(device):
            received = coef[sources, send_ids[:, device, :]].reshape(DEVICES * SLOT, RANK, NRHS)
            picked = received[far_list[device]].reshape(LD, fanout, RANK, NRHS)
            coupling = lax.dynamic_slice_in_dim(far_coupling, device * LD, LD, 0)
            trans = jnp.einsum('lfab,lfbs->las', coupling.astype(jnp.float32), picked.astype(jnp.float32)).astype(jnp.bfloat16)
            target = lax.dynamic_slice_in_dim(target_basis, device * ROWS, ROWS, 0).reshape(LD, LEAF, RANK)
            far = jnp.einsum('lia,las->lis', target.astype(jnp.float32), trans.astype(jnp.float32)).reshape(ROWS, NRHS)
            near_rows = lax.dynamic_slice_in_dim(near_blocks, device * ROWS, ROWS, 0)
            return near_apply(near_rows, ext_all[device]) + far
        extra = lax.map(one_device, jnp.arange(DEVICES, dtype=jnp.int32))
        return resid + extra.reshape(DEVICES * ROWS, NRHS)
    solution = jnp.zeros_like(rhs)
    residual = rhs
    for step in range(ITERS):
        image = apply(residual)
        gram = jnp.einsum('rs,rt->st', image, image, precision=lax.Precision.HIGHEST)
        proj = jnp.einsum('rs,rt->st', image, residual, precision=lax.Precision.HIGHEST)
        factor = jnp.linalg.cholesky(gram)
        alpha = jax.scipy.linalg.cho_solve((factor, True), proj)
        solution = solution + jnp.dot(residual, alpha, precision=lax.Precision.HIGHEST)
        residual = residual - jnp.dot(image, alpha, precision=lax.Precision.HIGHEST)
    return (solution, residual)
```

```python
import jax
import jax.numpy as jnp
from jax import lax
from jax.experimental import pallas as pl
from jax.experimental.pallas import tpu as pltpu
from jax.sharding import Mesh
from jax.sharding import PartitionSpec as P

NEAR = 1024
HALO = 256
LEAF = 128
RANK = 64
WIDTH = 256
TILE = 512
BLK = ("blk_0", "blk_1")
WIDE_BLK = ("wide_0", "wide_1", "blk_0", "blk_1")
F32 = jnp.float32
BF16 = jnp.bfloat16
HIGHEST = lax.Precision.HIGHEST


def params(mib):
    return pltpu.CompilerParams(
        dimension_semantics=("arbitrary",), vmem_limit_bytes=mib * 1024 * 1024
    )


def whole(*shape):
    return pl.BlockSpec(shape, lambda t: (0,) * len(shape))


def tiled(*shape):
    return pl.BlockSpec(shape, lambda t: (t,) + (0,) * (len(shape) - 1))


def smem():
    return pl.BlockSpec(memory_space=pltpu.SMEM)


def hbm():
    return pl.BlockSpec(memory_space=pltpu.HBM)


def dot(a, b):
    return jnp.dot(a, b, preferred_element_type=F32)


def dot_t(a, b):
    return lax.dot_general(a, b, (((0,), (0,)), ((), ())), preferred_element_type=F32)


def halves(x):
    hi = x.astype(BF16)
    return hi, (x - hi.astype(F32)).astype(BF16)


def dot3(x, hi, lo):
    xh, xl = halves(x)
    return dot(xh, hi) + (dot(xl, hi) + dot(xh, lo))


def send_rows(packed, ids, out, sem, count):
    def one(d, carry):
        pltpu.make_async_copy(packed.at[ids[d]], out.at[d], sem).start()
        return carry

    lax.fori_loop(0, count, one, 0, unroll=8)
    pltpu.make_async_copy(out, out, sem).wait()


def front_kernel(ids, r, s, out, packed, sem):
    t = pl.program_id(0)
    vb = r[...].astype(BF16)
    per = TILE // LEAF
    for i in range(per):
        rows = slice(i * LEAF, (i + 1) * LEAF)
        packed[t * per + i] = dot_t(s[rows], vb[rows]).astype(BF16)

    @pl.when(t == pl.num_programs(0) - 1)
    def _():
        send_rows(packed, ids, out, sem, out.shape[0])


def front(ids, r, s):
    rows = r.shape[0]
    count = ids.shape[0]
    return pl.pallas_call(
        front_kernel,
        grid=(rows // TILE,),
        in_specs=[smem(), tiled(TILE, WIDTH), tiled(TILE, RANK)],
        out_specs=hbm(),
        out_shape=jax.ShapeDtypeStruct((count, RANK, WIDTH), BF16),
        scratch_shapes=[
            pltpu.VMEM((rows // LEAF, RANK, WIDTH), BF16),
            pltpu.SemaphoreType.DMA(()),
        ],
        compiler_params=params(16),
        name="front",
    )(ids, r, s)


def near0_kernel(r, lo, hi, near, s, base, err, ext):
    t = pl.program_id(0)
    rows = r.shape[0]

    @pl.when(t == 0)
    def _():
        ext[:HALO] = lo[...].astype(BF16)
        ext[HALO : HALO + rows] = r[...].astype(BF16)
        ext[HALO + rows :] = hi[...].astype(BF16)

    first = pl.multiple_of((t // (NEAR // TILE)) * NEAR, NEAR)
    own = r[pl.ds(pl.multiple_of(t * TILE, TILE), TILE)]
    base[...] = own + dot(near[...], ext[pl.ds(first, NEAR + 2 * HALO)])
    rh, rl = halves(own)
    for i in range(TILE // LEAF):
        cut = slice(i * LEAF, (i + 1) * LEAF)
        high = dot_t(s[cut], rh[cut])
        low = dot_t(s[cut], rl[cut])
        err[i] = (high.astype(BF16).astype(F32) - high) - low


def near0(r, lo, hi, near, s):
    rows = r.shape[0]
    per = TILE // LEAF
    return pl.pallas_call(
        near0_kernel,
        grid=(rows // TILE,),
        in_specs=[
            whole(rows, WIDTH),
            whole(HALO, WIDTH),
            whole(HALO, WIDTH),
            tiled(TILE, NEAR + 2 * HALO),
            tiled(TILE, RANK),
        ],
        out_specs=[tiled(TILE, WIDTH), tiled(per, RANK, WIDTH)],
        out_shape=[
            jax.ShapeDtypeStruct((rows, WIDTH), F32),
            jax.ShapeDtypeStruct((rows // LEAF, RANK, WIDTH), F32),
        ],
        scratch_shapes=[pltpu.VMEM((rows + 2 * HALO, WIDTH), BF16)],
        compiler_params=params(32),
        cost_estimate=pl.CostEstimate(flops=4_000_000_000, bytes_accessed=24_000_000, transcendentals=0),
        name="near0",
    )(r, lo, hi, near, s)


def gram_step(t, image, r, acc):
    ih, il = halves(image)
    rh, rl = halves(r)

    @pl.when(t == 0)
    def _():
        acc[...] = jnp.zeros(acc.shape, F32)

    turned = ih.T
    left = jnp.concatenate([turned, turned, il.T], axis=1)
    gram = jnp.concatenate([ih, il, ih], axis=0)
    proj = jnp.concatenate([rh, rl, rh], axis=0)
    acc[...] += dot(left, jnp.concatenate([gram, proj], axis=1))
    return ih, il


def gram_end(acc, out):
    for i in range(WIDTH // 8):
        cut = slice(8 * i, 8 * i + 8)
        for h in range(2):
            out[2 * i + h] = acc[cut, 128 * h : 128 * h + 128]
            out[64 + 2 * i + h] = acc[cut, WIDTH + 128 * h : WIDTH + 128 * h + 128]


def slots_of(readers, incoming, leaf):
    return jnp.concatenate([incoming[readers[leaf * 4 + f]] for f in range(4)], axis=0)


def far0_kernel(ids, readers, incoming, coup, tb, s, base, r, err, image, trans, gp, out, packed, direct, acc, sem):
    t = pl.program_id(0)
    per = TILE // LEAF
    tiles = []
    for i in range(per):
        cut = slice(i * LEAF, (i + 1) * LEAF)
        tr = dot(coup[i * RANK : (i + 1) * RANK], slots_of(readers, incoming, t * per + i))
        trans[i * RANK : (i + 1) * RANK] = tr
        tiles.append(base[cut] + dot(tb[cut], tr.astype(BF16)))
    value = jnp.concatenate(tiles, axis=0)
    image[...] = value
    ih, il = gram_step(t, value, r[...], acc)
    for i in range(per):
        cut = slice(i * LEAF, (i + 1) * LEAF)
        direct[t * per + i] = dot_t(s[cut], ih[cut]) + dot_t(s[cut], il[cut])

    @pl.when(t == pl.num_programs(0) - 1)
    def _():
        gram_end(acc, gp)
        gram, total = acc[:, :WIDTH], acc[:, WIDTH:]
        eye = lax.broadcasted_iota(jnp.int32, gram.shape, 0) == lax.broadcasted_iota(jnp.int32, gram.shape, 1)
        g = jnp.sum(jnp.where(eye, gram, 0.0), axis=0, keepdims=True)
        p = jnp.sum(jnp.where(eye, total, 0.0), axis=0, keepdims=True)
        fits = (4.0 * p > g) & (4.0 * g > p)
        guess = jnp.where(fits, g / jnp.where(fits, p, 1.0), 0.0)
        for leaf in range(packed.shape[0]):
            packed[leaf] = (direct[leaf] + err[leaf] * guess).astype(BF16)
        send_rows(packed, ids, out, sem, out.shape[0])


def far0(ids, readers, incoming, coup, tb, s, base, r, err):
    rows = r.shape[0]
    leaves = rows // LEAF
    count = ids.shape[0]
    per = TILE // LEAF
    return pl.pallas_call(
        far0_kernel,
        grid=(rows // TILE,),
        in_specs=[
            smem(),
            smem(),
            whole(count, RANK, WIDTH),
            tiled(per * RANK, 4 * RANK),
            tiled(TILE, RANK),
            tiled(TILE, RANK),
            tiled(TILE, WIDTH),
            tiled(TILE, WIDTH),
            whole(leaves, RANK, WIDTH),
        ],
        out_specs=[tiled(TILE, WIDTH), tiled(per * RANK, WIDTH), whole(128, 8, 128), hbm()],
        out_shape=[
            jax.ShapeDtypeStruct((rows, WIDTH), F32),
            jax.ShapeDtypeStruct((leaves * RANK, WIDTH), F32),
            jax.ShapeDtypeStruct((128, 8, 128), F32),
            jax.ShapeDtypeStruct((count, RANK, WIDTH), BF16),
        ],
        scratch_shapes=[
            pltpu.VMEM((leaves, RANK, WIDTH), BF16),
            pltpu.VMEM((leaves, RANK, WIDTH), F32),
            pltpu.VMEM((WIDTH, 2 * WIDTH), F32),
            pltpu.SemaphoreType.DMA(()),
        ],
        compiler_params=params(40),
        name="far0",
    )(ids, readers, incoming, coup, tb, s, base, r, err)


def sum_kernel(parts, out):
    total = jnp.sum(parts[...], axis=0)
    out[...] = jnp.broadcast_to(total[None], out.shape)


def summed(parts):
    return pl.pallas_call(
        sum_kernel,
        out_shape=jax.ShapeDtypeStruct(parts.shape, F32),
        compiler_params=pltpu.CompilerParams(vmem_limit_bytes=8 * 1024 * 1024),
        name="summed",
    )(parts)


def lane(x, c):
    return jnp.broadcast_to(x[:, c : c + 1], (8, 128))


def sub(x, k):
    return jnp.broadcast_to(x[k : k + 1, :], (8, 128))


def inverse(rows):
    lanes = lax.broadcasted_iota(jnp.int32, (8, 128), 1)
    subs = lax.broadcasted_iota(jnp.int32, (8, 128), 0)
    rows = list(rows)
    count = len(rows)
    for p in range(count):
        pivot = rows[p]
        cols = [lane(pivot, 8 * p + j) for j in range(8)]
        for k in range(8):
            inv = 1.0 / sub(cols[k], k)
            ck = cols[k]
            here = subs == k
            scaled = sub(pivot, k) * inv
            pivot = jnp.where(here, scaled, pivot - ck * scaled)
            for j in range(8):
                if j != k:
                    cj = sub(cols[j], k) * inv
                    cols[j] = jnp.where(here, cj, cols[j] - ck * cj)
            cols[k] = jnp.where(here, inv, -ck * inv)
            pivot = jnp.where(lanes == 8 * p + k, cols[k], pivot)
        spread = [sub(pivot, j) for j in range(8)]
        panel = (lanes >= 8 * p) & (lanes < 8 * p + 8)
        for i in range(count):
            if i != p:
                value = jnp.where(panel, 0.0, rows[i])
                for j in range(8):
                    value = value - lane(rows[i], 8 * p + j) * spread[j]
                rows[i] = value
        rows[p] = pivot
    return rows


def exact(a, b):
    return jnp.dot(a, b, preferred_element_type=F32, precision=HIGHEST)


def solve_kernel(gp, alpha, high, low):
    def block(first, i0, i1, h):
        return jnp.concatenate([gp[first + 2 * i + h] for i in range(i0, i1)], axis=0)

    x11 = jnp.concatenate(inverse([gp[2 * i] for i in range(16)]), axis=0)
    a12 = block(0, 0, 16, 1)
    a21 = block(0, 16, 32, 0)
    w = exact(x11, a12)
    b1 = jnp.concatenate([block(64, 0, 16, 0), block(64, 0, 16, 1)], axis=1)
    b2 = jnp.concatenate([block(64, 16, 32, 0), block(64, 16, 32, 1)], axis=1)
    schur = block(0, 16, 32, 1) - exact(a21, w)
    y1 = exact(x11, b1)
    z = b2 - exact(a21, y1)
    x22 = jnp.concatenate(inverse([schur[8 * i : 8 * i + 8] for i in range(16)]), axis=0)
    lower = exact(x22, z)
    upper = y1 - exact(w, lower)
    value = jnp.concatenate([upper, lower], axis=0)
    alpha[...] = value
    hi, lo = halves(value)
    high[...] = hi
    low[...] = lo


def solve(gp):
    return pl.pallas_call(
        solve_kernel,
        out_shape=[
            jax.ShapeDtypeStruct((WIDTH, WIDTH), F32),
            jax.ShapeDtypeStruct((WIDTH, WIDTH), BF16),
            jax.ShapeDtypeStruct((WIDTH, WIDTH), BF16),
        ],
        compiler_params=pltpu.CompilerParams(vmem_limit_bytes=16 * 1024 * 1024),
        cost_estimate=pl.CostEstimate(flops=12_000_000_000, bytes_accessed=1_000_000, transcendentals=0),
        name="solve",
    )(gp)


def near1_kernel(r, lo, hi, image, ilo, ihi, ah, al, near, resid, base, sol, ext, full):
    t = pl.program_id(0)
    rows = r.shape[0]
    high, low = ah[...], al[...]

    @pl.when(t == 0)
    def _():
        ext[:HALO] = (lo[...] - dot3(ilo[...], high, low)).astype(BF16)
        for c in range(rows // TILE):
            cut = slice(c * TILE, (c + 1) * TILE)
            value = r[cut] - dot3(image[cut], high, low)
            full[cut] = value
            ext[HALO + c * TILE : HALO + (c + 1) * TILE] = value.astype(BF16)
        ext[HALO + rows :] = (hi[...] - dot3(ihi[...], high, low)).astype(BF16)

    first = pl.multiple_of((t // (NEAR // TILE)) * NEAR, NEAR)
    here = pl.ds(pl.multiple_of(t * TILE, TILE), TILE)
    own = full[here]
    resid[...] = own
    base[...] = own + dot(near[...], ext[pl.ds(first, NEAR + 2 * HALO)])
    sol[...] = dot3(r[here], high, low)


def near1(r, lo, hi, image, ilo, ihi, ah, al, near):
    rows = r.shape[0]
    return pl.pallas_call(
        near1_kernel,
        grid=(rows // TILE,),
        in_specs=[
            whole(rows, WIDTH),
            whole(HALO, WIDTH),
            whole(HALO, WIDTH),
            whole(rows, WIDTH),
            whole(HALO, WIDTH),
            whole(HALO, WIDTH),
            whole(WIDTH, WIDTH),
            whole(WIDTH, WIDTH),
            tiled(TILE, NEAR + 2 * HALO),
        ],
        out_specs=[tiled(TILE, WIDTH)] * 3,
        out_shape=[jax.ShapeDtypeStruct((rows, WIDTH), F32)] * 3,
        scratch_shapes=[
            pltpu.VMEM((rows + 2 * HALO, WIDTH), BF16),
            pltpu.VMEM((rows, WIDTH), F32),
        ],
        compiler_params=params(48),
        cost_estimate=pl.CostEstimate(flops=8_000_000_000, bytes_accessed=36_000_000, transcendentals=0),
        name="near1",
    )(r, lo, hi, image, ilo, ihi, ah, al, near)


def far1_kernel(readers, incoming, coup, tb, base, r, trans, ah, al, image, gp, acc):
    t = pl.program_id(0)
    per = TILE // LEAF
    moved = jnp.concatenate(
        [
            dot(coup[i * RANK : (i + 1) * RANK], slots_of(readers, incoming, t * per + i))
            for i in range(per)
        ],
        axis=0,
    )
    tr = (trans[...] - dot3(moved, ah[...], al[...])).astype(BF16)
    tiles = []
    for i in range(per):
        cut = slice(i * LEAF, (i + 1) * LEAF)
        tiles.append(base[cut] + dot(tb[cut], tr[i * RANK : (i + 1) * RANK]))
    value = jnp.concatenate(tiles, axis=0)
    image[...] = value
    gram_step(t, value, r[...], acc)

    @pl.when(t == pl.num_programs(0) - 1)
    def _():
        gram_end(acc, gp)


def far1(readers, incoming, coup, tb, base, r, trans, ah, al):
    rows = r.shape[0]
    count = incoming.shape[0]
    per = TILE // LEAF
    return pl.pallas_call(
        far1_kernel,
        grid=(rows // TILE,),
        in_specs=[
            smem(),
            whole(count, RANK, WIDTH),
            tiled(per * RANK, 4 * RANK),
            tiled(TILE, RANK),
            tiled(TILE, WIDTH),
            tiled(TILE, WIDTH),
            tiled(per * RANK, WIDTH),
            whole(WIDTH, WIDTH),
            whole(WIDTH, WIDTH),
        ],
        out_specs=[tiled(TILE, WIDTH), whole(128, 8, 128)],
        out_shape=[
            jax.ShapeDtypeStruct((rows, WIDTH), F32),
            jax.ShapeDtypeStruct((128, 8, 128), F32),
        ],
        scratch_shapes=[
            pltpu.VMEM((WIDTH, 2 * WIDTH), F32),
        ],
        compiler_params=params(32),
        name="far1",
    )(readers, incoming, coup, tb, base, r, trans, ah, al)


def finish_kernel(sol, r, image, ah, al, solution, residual):
    high, low = ah[...], al[...]
    solution[...] = sol[...] + dot3(r[...], high, low)
    residual[...] = r[...] - dot3(image[...], high, low)


def finish(sol, r, image, ah, al):
    rows = r.shape[0]
    return pl.pallas_call(
        finish_kernel,
        grid=(rows // TILE,),
        in_specs=[tiled(TILE, WIDTH)] * 3 + [whole(WIDTH, WIDTH)] * 2,
        out_specs=[tiled(TILE, WIDTH)] * 2,
        out_shape=[jax.ShapeDtypeStruct((rows, WIDTH), F32)] * 2,
        compiler_params=params(16),
        name="finish",
    )(sol, r, image, ah, al)


def exchange(value):
    return lax.all_to_all(value, WIDE_BLK, split_axis=0, concat_axis=0, tiled=True)


def sides(value):
    count = lax.axis_size(BLK)
    up = [(i, (i + 1) % count) for i in range(count)]
    down = [(j, i) for i, j in up]
    before = lax.ppermute(value[-HALO:], BLK, up)
    after = lax.ppermute(value[:HALO], BLK, down)
    return before, after


def shards(rhs, near_blocks, source_basis, target_basis, far_coupling, send_ids, far_list):
    leaves = rhs.shape[0] // LEAF
    ids = send_ids.reshape(-1)
    readers = far_list.reshape(-1)
    coup = far_coupling.transpose(0, 2, 1, 3).reshape(leaves * RANK, 4 * RANK)
    lo, hi = sides(rhs)
    incoming = exchange(front(ids, rhs, source_basis))
    base0, err = near0(rhs, lo, hi, near_blocks, source_basis)
    image0, trans0, gp0, outgoing = far0(
        ids, readers, incoming, coup, target_basis, source_basis, base0, rhs, err
    )
    parts = exchange(gp0)
    ilo, ihi = sides(image0)
    total = summed(parts)
    total, outgoing = lax.optimization_barrier((total, outgoing))
    whole0 = exchange(total)
    incoming1 = exchange(outgoing)
    _, ah, al = solve(whole0)
    r1, base1, sol = near1(rhs, lo, hi, image0, ilo, ihi, ah, al, near_blocks)
    image1, gp1 = far1(readers, incoming1, coup, target_basis, base1, r1, trans0, ah, al)
    whole1 = exchange(summed(exchange(gp1)))
    _, bh, bl = solve(whole1)
    return tuple(finish(sol, r1, image1, bh, bl))


def solution(mesh):
    split = Mesh(mesh.devices.reshape(4, 2, 4, 4), ("wide_0", "wide_1", "blk_0", "blk_1"))
    return jax.shard_map(
        shards,
        mesh=split,
        in_specs=(
            P(WIDE_BLK, None),
            P(WIDE_BLK, None),
            P(WIDE_BLK, None),
            P(WIDE_BLK, None),
            P(WIDE_BLK, None, None, None),
            P(WIDE_BLK, None, None),
            P(WIDE_BLK, None),
        ),
        out_specs=(P(WIDE_BLK, None), P(WIDE_BLK, None)),
        check_vma=False,
    )
```

```python
import jax
import jax.numpy as jnp
from jax import lax
from jax.experimental import pallas as pl
from jax.experimental.pallas import tpu as pltpu
from jax.sharding import Mesh
from jax.sharding import PartitionSpec as P

NEAR = 1024
HALO = 256
LEAF = 128
RANK = 64
WIDTH = 256
TILE = 512
FULL = 58
BLK = ("blk_0", "blk_1")
WIDE_BLK = ("wide_0", "wide_1", "blk_0", "blk_1")
F32 = jnp.float32
BF16 = jnp.bfloat16
HIGHEST = lax.Precision.HIGHEST


def params(mib):
    return pltpu.CompilerParams(
        dimension_semantics=("arbitrary",), vmem_limit_bytes=mib * 1024 * 1024
    )


def whole(*shape):
    return pl.BlockSpec(shape, lambda t: (0,) * len(shape))


def tiled(*shape):
    return pl.BlockSpec(shape, lambda t: (t,) + (0,) * (len(shape) - 1))


def across(rows, cols):
    return pl.BlockSpec((rows, cols), lambda t: (0, t))


def smem():
    return pl.BlockSpec(memory_space=pltpu.SMEM)


def hbm():
    return pl.BlockSpec(memory_space=pltpu.HBM)


def dot(a, b):
    return jnp.dot(a, b, preferred_element_type=F32)


def dot_t(a, b):
    return lax.dot_general(a, b, (((0,), (0,)), ((), ())), preferred_element_type=F32)


def halves(x):
    hi = x.astype(BF16)
    return hi, (x - hi.astype(F32)).astype(BF16)


def dot3(x, hi, lo):
    xh, xl = halves(x)
    return dot(xh, hi) + (dot(xl, hi) + dot(xh, lo))


def send_rows(packed, ids, out, sem, count):
    def one(d, carry):
        pltpu.make_async_copy(packed.at[ids[d]], out.at[d], sem).start()
        return carry

    lax.fori_loop(0, count, one, 0, unroll=8)
    pltpu.make_async_copy(out, out, sem).wait()


def front_kernel(ids, r, s, out, packed, sem):
    t = pl.program_id(0)
    vb = r[...].astype(BF16)
    per = TILE // LEAF
    for i in range(per):
        rows = slice(i * LEAF, (i + 1) * LEAF)
        packed[t * per + i] = dot(s[:, rows], vb[rows]).astype(BF16)

    @pl.when(t == pl.num_programs(0) - 1)
    def _():
        send_rows(packed, ids, out, sem, out.shape[0])


def front(ids, r, s):
    rows = r.shape[0]
    count = ids.shape[0]
    return pl.pallas_call(
        front_kernel,
        grid=(rows // TILE,),
        in_specs=[smem(), tiled(TILE, WIDTH), across(RANK, TILE)],
        out_specs=hbm(),
        out_shape=jax.ShapeDtypeStruct((count, RANK, WIDTH), BF16),
        scratch_shapes=[
            pltpu.VMEM((rows // LEAF, RANK, WIDTH), BF16),
            pltpu.SemaphoreType.DMA(()),
        ],
        compiler_params=params(FULL),
        name="front",
    )(ids, r, s)


def near0_kernel(r, near, s, base, err, ext):
    t = pl.program_id(0)
    rows = r.shape[0]

    @pl.when(t == 0)
    def _():
        ext[:HALO] = jnp.zeros((HALO, WIDTH), BF16)
        ext[HALO : HALO + rows] = r[...].astype(BF16)
        ext[HALO + rows :] = jnp.zeros((HALO, WIDTH), BF16)

    first = pl.multiple_of((t // (NEAR // TILE)) * NEAR, NEAR)
    own = r[pl.ds(pl.multiple_of(t * TILE, TILE), TILE)]
    base[...] = own + dot(near[...], ext[pl.ds(first, NEAR + 2 * HALO)])
    rh, rl = halves(own)
    for i in range(TILE // LEAF):
        cut = slice(i * LEAF, (i + 1) * LEAF)
        high = dot(s[:, cut], rh[cut])
        low = dot(s[:, cut], rl[cut])
        err[i] = (high.astype(BF16).astype(F32) - high) - low


def near0(r, near, s):
    rows = r.shape[0]
    per = TILE // LEAF
    return pl.pallas_call(
        near0_kernel,
        grid=(rows // TILE,),
        in_specs=[
            whole(rows, WIDTH),
            tiled(TILE, NEAR + 2 * HALO),
            across(RANK, TILE),
        ],
        out_specs=[tiled(TILE, WIDTH), tiled(per, RANK, WIDTH)],
        out_shape=[
            jax.ShapeDtypeStruct((rows, WIDTH), F32),
            jax.ShapeDtypeStruct((rows // LEAF, RANK, WIDTH), F32),
        ],
        scratch_shapes=[pltpu.VMEM((rows + 2 * HALO, WIDTH), BF16)],
        compiler_params=params(FULL),
        cost_estimate=pl.CostEstimate(flops=4_000_000_000, bytes_accessed=24_000_000, transcendentals=0),
        name="near0",
    )(r, near, s)


def gram_step(t, image, r, acc):
    ih, il = halves(image)
    rh, rl = halves(r)

    @pl.when(t == 0)
    def _():
        acc[...] = jnp.zeros(acc.shape, F32)

    turned = ih.T
    left = jnp.concatenate([turned, turned, il.T], axis=1)
    gram = jnp.concatenate([ih, il, ih], axis=0)
    proj = jnp.concatenate([rh, rl, rh], axis=0)
    acc[...] += dot(left, jnp.concatenate([gram, proj], axis=1))
    return ih, il


def gram_end(acc, out):
    for i in range(WIDTH // 8):
        cut = slice(8 * i, 8 * i + 8)
        for h in range(2):
            out[2 * i + h] = acc[cut, 128 * h : 128 * h + 128]
            out[64 + 2 * i + h] = acc[cut, WIDTH + 128 * h : WIDTH + 128 * h + 128]


def slots_of(readers, incoming, leaf):
    return jnp.concatenate([incoming[readers[leaf * 4 + f]] for f in range(4)], axis=0)


def edge_specs(tiles):
    edge = NEAR // TILE
    return [
        whole(HALO, WIDTH),
        whole(HALO, WIDTH),
        pl.BlockSpec((TILE, HALO), lambda t: (jnp.minimum(t, edge - 1), 0)),
        pl.BlockSpec((TILE, HALO), lambda t: (jnp.maximum(t, tiles - edge), (NEAR + HALO) // HALO)),
    ]


def add_edges(t, image, first, last, left, right):
    edge = NEAR // TILE

    @pl.when(t < edge)
    def _():
        image[...] += dot(left[...], first())

    @pl.when(t >= pl.num_programs(0) - edge)
    def _():
        image[...] += dot(right[...], last())


def far0_kernel(ids, readers, incoming, coup, tb, s, base, r, err, lo, hi, left, right, image, first, last, trans, gp, out, packed, direct, acc, sem):
    t = pl.program_id(0)
    per = TILE // LEAF
    tiles = []
    for i in range(per):
        cut = slice(i * LEAF, (i + 1) * LEAF)
        tr = dot(coup[i * RANK : (i + 1) * RANK], slots_of(readers, incoming, t * per + i))
        trans[i * RANK : (i + 1) * RANK] = tr
        tiles.append(base[cut] + dot(tb[cut], tr.astype(BF16)))
    image[...] = jnp.concatenate(tiles, axis=0)
    add_edges(t, image, lambda: lo[...].astype(BF16), lambda: hi[...].astype(BF16), left, right)

    @pl.when(t == 0)
    def _():
        first[...] = image[:HALO]

    @pl.when(t == pl.num_programs(0) - 1)
    def _():
        last[...] = image[TILE - HALO :]

    ih, il = gram_step(t, image[...], r[...], acc)
    for i in range(per):
        cut = slice(i * LEAF, (i + 1) * LEAF)
        direct[t * per + i] = dot(s[:, cut], ih[cut]) + dot(s[:, cut], il[cut])

    @pl.when(t == pl.num_programs(0) - 1)
    def _():
        gram_end(acc, gp)
        gram, total = acc[:, :WIDTH], acc[:, WIDTH:]
        eye = lax.broadcasted_iota(jnp.int32, gram.shape, 0) == lax.broadcasted_iota(jnp.int32, gram.shape, 1)
        g = jnp.sum(jnp.where(eye, gram, 0.0), axis=0, keepdims=True)
        p = jnp.sum(jnp.where(eye, total, 0.0), axis=0, keepdims=True)
        fits = (4.0 * p > g) & (4.0 * g > p)
        guess = jnp.where(fits, g / jnp.where(fits, p, 1.0), 0.0)
        for leaf in range(packed.shape[0]):
            packed[leaf] = (direct[leaf] + err[leaf] * guess).astype(BF16)
        send_rows(packed, ids, out, sem, out.shape[0])


def far0(ids, readers, incoming, coup, tb, s, base, r, err, lo, hi, near):
    rows = r.shape[0]
    leaves = rows // LEAF
    count = ids.shape[0]
    per = TILE // LEAF
    return pl.pallas_call(
        far0_kernel,
        grid=(rows // TILE,),
        in_specs=[
            smem(),
            smem(),
            whole(count, RANK, WIDTH),
            tiled(per * RANK, 4 * RANK),
            tiled(TILE, RANK),
            across(RANK, TILE),
            tiled(TILE, WIDTH),
            tiled(TILE, WIDTH),
            whole(leaves, RANK, WIDTH),
            *edge_specs(rows // TILE),
        ],
        out_specs=[
            tiled(TILE, WIDTH),
            whole(HALO, WIDTH),
            whole(HALO, WIDTH),
            tiled(per * RANK, WIDTH),
            whole(128, 8, 128),
            hbm(),
        ],
        out_shape=[
            jax.ShapeDtypeStruct((rows, WIDTH), F32),
            jax.ShapeDtypeStruct((HALO, WIDTH), F32),
            jax.ShapeDtypeStruct((HALO, WIDTH), F32),
            jax.ShapeDtypeStruct((leaves * RANK, WIDTH), F32),
            jax.ShapeDtypeStruct((128, 8, 128), F32),
            jax.ShapeDtypeStruct((count, RANK, WIDTH), BF16),
        ],
        scratch_shapes=[
            pltpu.VMEM((leaves, RANK, WIDTH), BF16),
            pltpu.VMEM((leaves, RANK, WIDTH), F32),
            pltpu.VMEM((WIDTH, 2 * WIDTH), F32),
            pltpu.SemaphoreType.DMA(()),
        ],
        compiler_params=params(FULL),
        name="far0",
    )(ids, readers, incoming, coup, tb, s, base, r, err, lo, hi, near, near)


def sum_kernel(parts, out):
    total = jnp.sum(parts[...], axis=0)
    out[...] = jnp.broadcast_to(total[None], out.shape)


def summed(parts):
    return pl.pallas_call(
        sum_kernel,
        out_shape=jax.ShapeDtypeStruct(parts.shape, F32),
        compiler_params=pltpu.CompilerParams(vmem_limit_bytes=8 * 1024 * 1024),
        name="summed",
    )(parts)


def lane(x, c):
    return jnp.broadcast_to(x[:, c : c + 1], (8, 128))


def sub(x, k):
    return jnp.broadcast_to(x[k : k + 1, :], (8, 128))


def inverse(rows):
    lanes = lax.broadcasted_iota(jnp.int32, (8, 128), 1)
    subs = lax.broadcasted_iota(jnp.int32, (8, 128), 0)
    rows = list(rows)
    count = len(rows)
    for p in range(count):
        pivot = rows[p]
        cols = [lane(pivot, 8 * p + j) for j in range(8)]
        for k in range(8):
            inv = 1.0 / sub(cols[k], k)
            ck = cols[k]
            here = subs == k
            scaled = sub(pivot, k) * inv
            pivot = jnp.where(here, scaled, pivot - ck * scaled)
            for j in range(8):
                if j != k:
                    cj = sub(cols[j], k) * inv
                    cols[j] = jnp.where(here, cj, cols[j] - ck * cj)
            cols[k] = jnp.where(here, inv, -ck * inv)
            pivot = jnp.where(lanes == 8 * p + k, cols[k], pivot)
        spread = [sub(pivot, j) for j in range(8)]
        panel = (lanes >= 8 * p) & (lanes < 8 * p + 8)
        for i in range(count):
            if i != p:
                value = jnp.where(panel, 0.0, rows[i])
                for j in range(8):
                    value = value - lane(rows[i], 8 * p + j) * spread[j]
                rows[i] = value
        rows[p] = pivot
    return rows


def exact(a, b):
    return jnp.dot(a, b, preferred_element_type=F32, precision=HIGHEST)


def solve_kernel(gp, alpha, high, low):
    def block(first, i0, i1, h):
        return jnp.concatenate([gp[first + 2 * i + h] for i in range(i0, i1)], axis=0)

    x11 = jnp.concatenate(inverse([gp[2 * i] for i in range(16)]), axis=0)
    a12 = block(0, 0, 16, 1)
    a21 = block(0, 16, 32, 0)
    w = exact(x11, a12)
    b1 = jnp.concatenate([block(64, 0, 16, 0), block(64, 0, 16, 1)], axis=1)
    b2 = jnp.concatenate([block(64, 16, 32, 0), block(64, 16, 32, 1)], axis=1)
    schur = block(0, 16, 32, 1) - exact(a21, w)
    y1 = exact(x11, b1)
    z = b2 - exact(a21, y1)
    x22 = jnp.concatenate(inverse([schur[8 * i : 8 * i + 8] for i in range(16)]), axis=0)
    lower = exact(x22, z)
    upper = y1 - exact(w, lower)
    value = jnp.concatenate([upper, lower], axis=0)
    alpha[...] = value
    hi, lo = halves(value)
    high[...] = hi
    low[...] = lo


def solve(gp):
    return pl.pallas_call(
        solve_kernel,
        out_shape=[
            jax.ShapeDtypeStruct((WIDTH, WIDTH), F32),
            jax.ShapeDtypeStruct((WIDTH, WIDTH), BF16),
            jax.ShapeDtypeStruct((WIDTH, WIDTH), BF16),
        ],
        compiler_params=pltpu.CompilerParams(vmem_limit_bytes=16 * 1024 * 1024),
        cost_estimate=pl.CostEstimate(flops=12_000_000_000, bytes_accessed=1_000_000, transcendentals=0),
        name="solve",
    )(gp)


def near1_kernel(r, image, ah, al, near, resid, base, sol, ext, full):
    t = pl.program_id(0)
    rows = r.shape[0]
    high, low = ah[...], al[...]

    @pl.when(t == 0)
    def _():
        ext[:HALO] = jnp.zeros((HALO, WIDTH), BF16)
        for c in range(rows // TILE):
            cut = slice(c * TILE, (c + 1) * TILE)
            value = r[cut] - dot3(image[cut], high, low)
            full[cut] = value
            ext[HALO + c * TILE : HALO + (c + 1) * TILE] = value.astype(BF16)
        ext[HALO + rows :] = jnp.zeros((HALO, WIDTH), BF16)

    first = pl.multiple_of((t // (NEAR // TILE)) * NEAR, NEAR)
    here = pl.ds(pl.multiple_of(t * TILE, TILE), TILE)
    own = full[here]
    resid[...] = own
    base[...] = own + dot(near[...], ext[pl.ds(first, NEAR + 2 * HALO)])
    sol[...] = dot3(r[here], high, low)


def near1(r, image, ah, al, near):
    rows = r.shape[0]
    return pl.pallas_call(
        near1_kernel,
        grid=(rows // TILE,),
        in_specs=[
            whole(rows, WIDTH),
            whole(rows, WIDTH),
            whole(WIDTH, WIDTH),
            whole(WIDTH, WIDTH),
            tiled(TILE, NEAR + 2 * HALO),
        ],
        out_specs=[tiled(TILE, WIDTH)] * 3,
        out_shape=[jax.ShapeDtypeStruct((rows, WIDTH), F32)] * 3,
        scratch_shapes=[
            pltpu.VMEM((rows + 2 * HALO, WIDTH), BF16),
            pltpu.VMEM((rows, WIDTH), F32),
        ],
        compiler_params=params(FULL),
        cost_estimate=pl.CostEstimate(flops=8_000_000_000, bytes_accessed=36_000_000, transcendentals=0),
        name="near1",
    )(r, image, ah, al, near)


def far1_kernel(readers, incoming, coup, tb, base, r, trans, ah, al, lo, hi, ilo, ihi, left, right, image, gp, acc):
    t = pl.program_id(0)
    per = TILE // LEAF
    moved = jnp.concatenate(
        [
            dot(coup[i * RANK : (i + 1) * RANK], slots_of(readers, incoming, t * per + i))
            for i in range(per)
        ],
        axis=0,
    )
    tr = (trans[...] - dot3(moved, ah[...], al[...])).astype(BF16)
    tiles = []
    for i in range(per):
        cut = slice(i * LEAF, (i + 1) * LEAF)
        tiles.append(base[cut] + dot(tb[cut], tr[i * RANK : (i + 1) * RANK]))
    image[...] = jnp.concatenate(tiles, axis=0)
    add_edges(
        t,
        image,
        lambda: (lo[...] - dot3(ilo[...], ah[...], al[...])).astype(BF16),
        lambda: (hi[...] - dot3(ihi[...], ah[...], al[...])).astype(BF16),
        left,
        right,
    )
    gram_step(t, image[...], r[...], acc)

    @pl.when(t == pl.num_programs(0) - 1)
    def _():
        gram_end(acc, gp)


def far1(readers, incoming, coup, tb, base, r, trans, ah, al, lo, hi, ilo, ihi, near):
    rows = r.shape[0]
    count = incoming.shape[0]
    per = TILE // LEAF
    return pl.pallas_call(
        far1_kernel,
        grid=(rows // TILE,),
        in_specs=[
            smem(),
            whole(count, RANK, WIDTH),
            tiled(per * RANK, 4 * RANK),
            tiled(TILE, RANK),
            tiled(TILE, WIDTH),
            tiled(TILE, WIDTH),
            tiled(per * RANK, WIDTH),
            whole(WIDTH, WIDTH),
            whole(WIDTH, WIDTH),
            whole(HALO, WIDTH),
            whole(HALO, WIDTH),
            *edge_specs(rows // TILE),
        ],
        out_specs=[tiled(TILE, WIDTH), whole(128, 8, 128)],
        out_shape=[
            jax.ShapeDtypeStruct((rows, WIDTH), F32),
            jax.ShapeDtypeStruct((128, 8, 128), F32),
        ],
        scratch_shapes=[
            pltpu.VMEM((WIDTH, 2 * WIDTH), F32),
        ],
        compiler_params=params(FULL),
        name="far1",
    )(readers, incoming, coup, tb, base, r, trans, ah, al, lo, hi, ilo, ihi, near, near)


def finish_kernel(sol, r, image, ah, al, solution, residual):
    high, low = ah[...], al[...]
    solution[...] = sol[...] + dot3(r[...], high, low)
    residual[...] = r[...] - dot3(image[...], high, low)


def finish(sol, r, image, ah, al):
    rows = r.shape[0]
    return pl.pallas_call(
        finish_kernel,
        grid=(rows // TILE,),
        in_specs=[tiled(TILE, WIDTH)] * 3 + [whole(WIDTH, WIDTH)] * 2,
        out_specs=[tiled(TILE, WIDTH)] * 2,
        out_shape=[jax.ShapeDtypeStruct((rows, WIDTH), F32)] * 2,
        compiler_params=params(FULL),
        name="finish",
    )(sol, r, image, ah, al)


def exchange(value):
    return lax.all_to_all(value, WIDE_BLK, split_axis=0, concat_axis=0, tiled=True)


def sides(first, last):
    count = lax.axis_size(BLK)
    up = [(i, (i + 1) % count) for i in range(count)]
    down = [(j, i) for i, j in up]
    return lax.ppermute(last, BLK, up), lax.ppermute(first, BLK, down)


def shards(rhs, near_blocks, source_basis, target_basis, far_coupling, send_ids, far_list):
    leaves = rhs.shape[0] // LEAF
    ids = send_ids.reshape(-1)
    readers = far_list.reshape(-1)
    source = source_basis.T
    incoming = exchange(front(ids, rhs, source))
    coup = far_coupling.transpose(0, 2, 1, 3).reshape(leaves * RANK, 4 * RANK)
    lo, hi = sides(rhs[:HALO], rhs[-HALO:])
    base0, err = near0(rhs, near_blocks, source)
    image0, first0, last0, trans0, gp0, outgoing = far0(
        ids, readers, incoming, coup, target_basis, source, base0, rhs, err, lo, hi, near_blocks
    )
    total = summed(exchange(gp0))
    total, outgoing = lax.optimization_barrier((total, outgoing))
    whole0 = exchange(total)
    incoming1 = exchange(outgoing)
    ilo, ihi = sides(first0, last0)
    _, ah, al = solve(whole0)
    r1, base1, sol = near1(rhs, image0, ah, al, near_blocks)
    image1, gp1 = far1(
        readers, incoming1, coup, target_basis, base1, r1, trans0, ah, al, lo, hi, ilo, ihi, near_blocks
    )
    whole1 = exchange(summed(exchange(gp1)))
    _, bh, bl = solve(whole1)
    return tuple(finish(sol, r1, image1, bh, bl))


def solution(mesh):
    split = Mesh(mesh.devices.reshape(4, 2, 4, 4), ("wide_0", "wide_1", "blk_0", "blk_1"))
    return jax.shard_map(
        shards,
        mesh=split,
        in_specs=(
            P(WIDE_BLK, None),
            P(WIDE_BLK, None),
            P(WIDE_BLK, None),
            P(WIDE_BLK, None),
            P(WIDE_BLK, None, None, None),
            P(WIDE_BLK, None, None),
            P(WIDE_BLK, None),
        ),
        out_specs=(P(WIDE_BLK, None), P(WIDE_BLK, None)),
        check_vma=False,
    )
```

```python
import jax
import jax.numpy as jnp
from jax import lax
from jax.experimental import pallas as pl
from jax.experimental.pallas import tpu as pltpu
from jax.sharding import Mesh
from jax.sharding import PartitionSpec as P

NEAR = 1024
HALO = 256
LEAF = 128
RANK = 64
WIDTH = 256
TILE = 512
FULL = 58
BLK = ("blk_0", "blk_1")
WIDE_BLK = ("wide_0", "wide_1", "blk_0", "blk_1")
F32 = jnp.float32
BF16 = jnp.bfloat16
HIGHEST = lax.Precision.HIGHEST


def params(mib):
    return pltpu.CompilerParams(
        dimension_semantics=("arbitrary",), vmem_limit_bytes=mib * 1024 * 1024
    )


def whole(*shape):
    return pl.BlockSpec(shape, lambda t: (0,) * len(shape), pipeline_mode=pl.Buffered(1))


def kept(*shape):
    return pl.BlockSpec(shape, lambda t: (0,) * len(shape))


def tiled(*shape):
    return pl.BlockSpec(shape, lambda t: (t,) + (0,) * (len(shape) - 1))


def across(rows, cols):
    return pl.BlockSpec((rows, cols), lambda t: (0, t))


def smem():
    return pl.BlockSpec(memory_space=pltpu.SMEM)


def hbm():
    return pl.BlockSpec(memory_space=pltpu.HBM)


def dot(a, b):
    return jnp.dot(a, b, preferred_element_type=F32)


def dot_t(a, b):
    return lax.dot_general(a, b, (((0,), (0,)), ((), ())), preferred_element_type=F32)


def halves(x):
    hi = x.astype(BF16)
    return hi, (x - hi.astype(F32)).astype(BF16)


def dot3(x, hi, lo):
    xh, xl = halves(x)
    return dot(xh, hi) + (dot(xl, hi) + dot(xh, lo))


def send_rows(packed, ids, out, sem, count):
    def one(d, carry):
        pltpu.make_async_copy(packed.at[ids[d]], out.at[d], sem).start()
        return carry

    lax.fori_loop(0, count, one, 0, unroll=8)
    pltpu.make_async_copy(out, out, sem).wait()


def front_kernel(ids, r, s, out, packed, sem):
    t = pl.program_id(0)
    vb = r[...].astype(BF16)
    per = TILE // LEAF
    for i in range(per):
        rows = slice(i * LEAF, (i + 1) * LEAF)
        packed[t * per + i] = dot(s[:, rows], vb[rows]).astype(BF16)

    @pl.when(t == pl.num_programs(0) - 1)
    def _():
        send_rows(packed, ids, out, sem, out.shape[0])


def front(ids, r, s):
    rows = r.shape[0]
    count = ids.shape[0]
    return pl.pallas_call(
        front_kernel,
        grid=(rows // TILE,),
        in_specs=[smem(), tiled(TILE, WIDTH), across(RANK, TILE)],
        out_specs=hbm(),
        out_shape=pltpu.HBM((count, RANK, WIDTH), BF16),
        scratch_shapes=[
            pltpu.VMEM((rows // LEAF, RANK, WIDTH), BF16),
            pltpu.SemaphoreType.DMA(()),
        ],
        compiler_params=params(FULL),
        name="front",
    )(ids, r, s)


def near0_kernel(r, near, s, base, err, ext):
    t = pl.program_id(0)
    rows = r.shape[0]

    @pl.when(t == 0)
    def _():
        ext[:HALO] = jnp.zeros((HALO, WIDTH), BF16)
        ext[HALO : HALO + rows] = r[...].astype(BF16)
        ext[HALO + rows :] = jnp.zeros((HALO, WIDTH), BF16)

    first = pl.multiple_of((t // (NEAR // TILE)) * NEAR, NEAR)
    own = r[pl.ds(pl.multiple_of(t * TILE, TILE), TILE)]
    base[...] = own + dot(near[...], ext[pl.ds(first, NEAR + 2 * HALO)])
    rh, rl = halves(own)
    for i in range(TILE // LEAF):
        cut = slice(i * LEAF, (i + 1) * LEAF)
        high = dot(s[:, cut], rh[cut])
        low = dot(s[:, cut], rl[cut])
        err[i] = (high.astype(BF16).astype(F32) - high) - low


def near0(r, near, s):
    rows = r.shape[0]
    per = TILE // LEAF
    return pl.pallas_call(
        near0_kernel,
        grid=(rows // TILE,),
        in_specs=[
            whole(rows, WIDTH),
            tiled(TILE, NEAR + 2 * HALO),
            across(RANK, TILE),
        ],
        out_specs=[tiled(TILE, WIDTH), tiled(per, RANK, WIDTH)],
        out_shape=[
            jax.ShapeDtypeStruct((rows, WIDTH), F32),
            jax.ShapeDtypeStruct((rows // LEAF, RANK, WIDTH), F32),
        ],
        scratch_shapes=[pltpu.VMEM((rows + 2 * HALO, WIDTH), BF16)],
        compiler_params=params(FULL),
        cost_estimate=pl.CostEstimate(flops=4_000_000_000, bytes_accessed=24_000_000, transcendentals=0),
        name="near0",
    )(r, near, s)


def gram_step(t, image, r, acc):
    ih, il = halves(image)
    rh, rl = halves(r)

    @pl.when(t == 0)
    def _():
        acc[...] = jnp.zeros(acc.shape, F32)

    high = jnp.concatenate([ih.T, rh.T], axis=0)
    low = jnp.concatenate([il.T, rl.T], axis=0)
    acc[...] += dot(jnp.concatenate([high, high, low], axis=1), jnp.concatenate([ih, il, ih], axis=0))
    return ih, il


def gram_end(acc, out):
    for i in range(2 * WIDTH // 8):
        for h in range(2):
            out[2 * i + h] = acc[8 * i : 8 * i + 8, 128 * h : 128 * h + 128]


def slots_of(readers, incoming, leaf):
    return jnp.concatenate([incoming[readers[leaf * 4 + f]] for f in range(4)], axis=0)


def edge_specs(tiles):
    edge = NEAR // TILE
    return [
        whole(HALO, WIDTH),
        whole(HALO, WIDTH),
        pl.BlockSpec((TILE, HALO), lambda t: (jnp.minimum(t, edge - 1), 0)),
        pl.BlockSpec((TILE, HALO), lambda t: (jnp.maximum(t - (tiles - edge), 0), 0)),
    ]


def add_edges(t, image, first, last, left, right):
    edge = NEAR // TILE

    @pl.when(t < edge)
    def _():
        image[...] += dot(left[...], first())

    @pl.when(t >= pl.num_programs(0) - edge)
    def _():
        image[...] += dot(right[...], last())


def far0_kernel(ids, readers, incoming, coup, tb, s, base, r, err, lo, hi, left, right, image, first, last, trans, gp, out, packed, direct, acc, sem):
    t = pl.program_id(0)
    per = TILE // LEAF
    tiles = []
    for i in range(per):
        cut = slice(i * LEAF, (i + 1) * LEAF)
        tr = dot(coup[i * RANK : (i + 1) * RANK], slots_of(readers, incoming, t * per + i))
        trans[i * RANK : (i + 1) * RANK] = tr
        tiles.append(base[cut] + dot(tb[cut], tr.astype(BF16)))
    image[...] = jnp.concatenate(tiles, axis=0)
    add_edges(t, image, lambda: lo[...].astype(BF16), lambda: hi[...].astype(BF16), left, right)

    @pl.when(t == 0)
    def _():
        first[...] = image[:HALO]

    @pl.when(t == pl.num_programs(0) - 1)
    def _():
        last[...] = image[TILE - HALO :]

    ih, il = gram_step(t, image[...], r[...], acc)
    for i in range(per):
        cut = slice(i * LEAF, (i + 1) * LEAF)
        direct[t * per + i] = dot(s[:, cut], ih[cut]) + dot(s[:, cut], il[cut])

    @pl.when(t == pl.num_programs(0) - 1)
    def _():
        gram_end(acc, gp)
        gram, total = acc[:WIDTH], acc[WIDTH:]
        eye = lax.broadcasted_iota(jnp.int32, gram.shape, 0) == lax.broadcasted_iota(jnp.int32, gram.shape, 1)
        g = jnp.sum(jnp.where(eye, gram, 0.0), axis=0, keepdims=True)
        p = jnp.sum(jnp.where(eye, total, 0.0), axis=0, keepdims=True)
        fits = (4.0 * p > g) & (4.0 * g > p)
        guess = jnp.where(fits, g / jnp.where(fits, p, 1.0), 0.0)
        for leaf in range(packed.shape[0]):
            packed[leaf] = (direct[leaf] + err[leaf] * guess).astype(BF16)
        send_rows(packed, ids, out, sem, out.shape[0])


def far0(ids, readers, incoming, coup, tb, s, base, r, err, lo, hi, left, right):
    rows = r.shape[0]
    leaves = rows // LEAF
    count = ids.shape[0]
    per = TILE // LEAF
    return pl.pallas_call(
        far0_kernel,
        grid=(rows // TILE,),
        in_specs=[
            smem(),
            smem(),
            whole(count, RANK, WIDTH),
            tiled(per * RANK, 4 * RANK),
            tiled(TILE, RANK),
            across(RANK, TILE),
            tiled(TILE, WIDTH),
            tiled(TILE, WIDTH),
            whole(leaves, RANK, WIDTH),
            *edge_specs(rows // TILE),
        ],
        out_specs=[
            tiled(TILE, WIDTH),
            kept(HALO, WIDTH),
            kept(HALO, WIDTH),
            tiled(per * RANK, WIDTH),
            kept(128, 8, 128),
            hbm(),
        ],
        out_shape=[
            jax.ShapeDtypeStruct((rows, WIDTH), F32),
            jax.ShapeDtypeStruct((HALO, WIDTH), F32),
            jax.ShapeDtypeStruct((HALO, WIDTH), F32),
            jax.ShapeDtypeStruct((leaves * RANK, WIDTH), F32),
            jax.ShapeDtypeStruct((128, 8, 128), F32),
            pltpu.HBM((count, RANK, WIDTH), BF16),
        ],
        scratch_shapes=[
            pltpu.VMEM((leaves, RANK, WIDTH), BF16),
            pltpu.VMEM((leaves, RANK, WIDTH), F32),
            pltpu.VMEM((2 * WIDTH, WIDTH), F32),
            pltpu.SemaphoreType.DMA(()),
        ],
        compiler_params=params(FULL),
        name="far0",
    )(ids, readers, incoming, coup, tb, s, base, r, err, lo, hi, left, right)


def sum_kernel(parts, out):
    total = jnp.sum(parts[...], axis=0)
    out[...] = jnp.broadcast_to(total[None], out.shape)


def summed(parts):
    return pl.pallas_call(
        sum_kernel,
        out_shape=jax.ShapeDtypeStruct(parts.shape, F32),
        compiler_params=pltpu.CompilerParams(vmem_limit_bytes=8 * 1024 * 1024),
        name="summed",
    )(parts)


def lane(x, c):
    return jnp.broadcast_to(x[:, c : c + 1], (8, 128))


def sub(x, k):
    return jnp.broadcast_to(x[k : k + 1, :], (8, 128))


def inverse(rows):
    lanes = lax.broadcasted_iota(jnp.int32, (8, 128), 1)
    subs = lax.broadcasted_iota(jnp.int32, (8, 128), 0)
    rows = list(rows)
    count = len(rows)
    for p in range(count):
        pivot = rows[p]
        cols = [lane(pivot, 8 * p + j) for j in range(8)]
        for k in range(8):
            inv = 1.0 / sub(cols[k], k)
            ck = cols[k]
            here = subs == k
            scaled = sub(pivot, k) * inv
            pivot = jnp.where(here, scaled, pivot - ck * scaled)
            for j in range(8):
                if j != k:
                    cj = sub(cols[j], k) * inv
                    cols[j] = jnp.where(here, cj, cols[j] - ck * cj)
            cols[k] = jnp.where(here, inv, -ck * inv)
            pivot = jnp.where(lanes == 8 * p + k, cols[k], pivot)
        spread = [sub(pivot, j) for j in range(8)]
        panel = (lanes >= 8 * p) & (lanes < 8 * p + 8)
        for i in range(count):
            if i != p:
                value = jnp.where(panel, 0.0, rows[i])
                for j in range(8):
                    value = value - lane(rows[i], 8 * p + j) * spread[j]
                rows[i] = value
        rows[p] = pivot
    return rows


def exact(a, b):
    return jnp.dot(a, b, preferred_element_type=F32, precision=HIGHEST)


def solve_kernel(gp, alpha, high, low):
    def block(first, i0, i1, h):
        return jnp.concatenate([gp[first + 2 * i + h] for i in range(i0, i1)], axis=0)

    x11 = jnp.concatenate(inverse([gp[2 * i] for i in range(16)]), axis=0)
    a12 = block(0, 0, 16, 1)
    a21 = block(0, 16, 32, 0)
    w = exact(x11, a12)
    b1 = block(64, 0, 32, 0).T
    b2 = block(64, 0, 32, 1).T
    schur = block(0, 16, 32, 1) - exact(a21, w)
    y1 = exact(x11, b1)
    z = b2 - exact(a21, y1)
    x22 = jnp.concatenate(inverse([schur[8 * i : 8 * i + 8] for i in range(16)]), axis=0)
    lower = exact(x22, z)
    upper = y1 - exact(w, lower)
    value = jnp.concatenate([upper, lower], axis=0)
    alpha[...] = value
    hi, lo = halves(value)
    high[...] = hi
    low[...] = lo


def solve(gp):
    return pl.pallas_call(
        solve_kernel,
        out_shape=[
            jax.ShapeDtypeStruct((WIDTH, WIDTH), F32),
            jax.ShapeDtypeStruct((WIDTH, WIDTH), BF16),
            jax.ShapeDtypeStruct((WIDTH, WIDTH), BF16),
        ],
        compiler_params=pltpu.CompilerParams(vmem_limit_bytes=16 * 1024 * 1024),
        cost_estimate=pl.CostEstimate(flops=12_000_000_000, bytes_accessed=1_000_000, transcendentals=0),
        name="solve",
    )(gp)


def near1_kernel(r, image, ah, al, near, resid, base, sol, ext, full):
    t = pl.program_id(0)
    rows = r.shape[0]
    high, low = ah[...], al[...]

    @pl.when(t == 0)
    def _():
        ext[:HALO] = jnp.zeros((HALO, WIDTH), BF16)
        for c in range(rows // TILE):
            cut = slice(c * TILE, (c + 1) * TILE)
            value = r[cut] - dot3(image[cut], high, low)
            full[cut] = value
            ext[HALO + c * TILE : HALO + (c + 1) * TILE] = value.astype(BF16)
        ext[HALO + rows :] = jnp.zeros((HALO, WIDTH), BF16)

    first = pl.multiple_of((t // (NEAR // TILE)) * NEAR, NEAR)
    here = pl.ds(pl.multiple_of(t * TILE, TILE), TILE)
    own = full[here]
    resid[...] = own
    base[...] = own + dot(near[...], ext[pl.ds(first, NEAR + 2 * HALO)])
    sol[...] = dot3(r[here], high, low)


def near1(r, image, ah, al, near):
    rows = r.shape[0]
    return pl.pallas_call(
        near1_kernel,
        grid=(rows // TILE,),
        in_specs=[
            whole(rows, WIDTH),
            whole(rows, WIDTH),
            whole(WIDTH, WIDTH),
            whole(WIDTH, WIDTH),
            tiled(TILE, NEAR + 2 * HALO),
        ],
        out_specs=[tiled(TILE, WIDTH)] * 3,
        out_shape=[jax.ShapeDtypeStruct((rows, WIDTH), F32)] * 3,
        scratch_shapes=[
            pltpu.VMEM((rows + 2 * HALO, WIDTH), BF16),
            pltpu.VMEM((rows, WIDTH), F32),
        ],
        compiler_params=params(FULL),
        cost_estimate=pl.CostEstimate(flops=8_000_000_000, bytes_accessed=36_000_000, transcendentals=0),
        name="near1",
    )(r, image, ah, al, near)


def far1_kernel(readers, incoming, coup, tb, base, r, trans, ah, al, lo, hi, ilo, ihi, left, right, image, gp, acc):
    t = pl.program_id(0)
    per = TILE // LEAF
    moved = jnp.concatenate(
        [
            dot(coup[i * RANK : (i + 1) * RANK], slots_of(readers, incoming, t * per + i))
            for i in range(per)
        ],
        axis=0,
    )
    tr = (trans[...] - dot3(moved, ah[...], al[...])).astype(BF16)
    tiles = []
    for i in range(per):
        cut = slice(i * LEAF, (i + 1) * LEAF)
        tiles.append(base[cut] + dot(tb[cut], tr[i * RANK : (i + 1) * RANK]))
    image[...] = jnp.concatenate(tiles, axis=0)
    add_edges(
        t,
        image,
        lambda: (lo[...] - dot3(ilo[...], ah[...], al[...])).astype(BF16),
        lambda: (hi[...] - dot3(ihi[...], ah[...], al[...])).astype(BF16),
        left,
        right,
    )
    gram_step(t, image[...], r[...], acc)

    @pl.when(t == pl.num_programs(0) - 1)
    def _():
        gram_end(acc, gp)


def far1(readers, incoming, coup, tb, base, r, trans, ah, al, lo, hi, ilo, ihi, left, right):
    rows = r.shape[0]
    count = incoming.shape[0]
    per = TILE // LEAF
    return pl.pallas_call(
        far1_kernel,
        grid=(rows // TILE,),
        in_specs=[
            smem(),
            whole(count, RANK, WIDTH),
            tiled(per * RANK, 4 * RANK),
            tiled(TILE, RANK),
            tiled(TILE, WIDTH),
            tiled(TILE, WIDTH),
            tiled(per * RANK, WIDTH),
            whole(WIDTH, WIDTH),
            whole(WIDTH, WIDTH),
            whole(HALO, WIDTH),
            whole(HALO, WIDTH),
            *edge_specs(rows // TILE),
        ],
        out_specs=[tiled(TILE, WIDTH), kept(128, 8, 128)],
        out_shape=[
            jax.ShapeDtypeStruct((rows, WIDTH), F32),
            jax.ShapeDtypeStruct((128, 8, 128), F32),
        ],
        scratch_shapes=[
            pltpu.VMEM((2 * WIDTH, WIDTH), F32),
        ],
        compiler_params=params(FULL),
        name="far1",
    )(readers, incoming, coup, tb, base, r, trans, ah, al, lo, hi, ilo, ihi, left, right)


def finish_kernel(sol, r, image, ah, al, solution, residual):
    high, low = ah[...], al[...]
    solution[...] = sol[...] + dot3(r[...], high, low)
    residual[...] = r[...] - dot3(image[...], high, low)


def finish(sol, r, image, ah, al):
    rows = r.shape[0]
    return pl.pallas_call(
        finish_kernel,
        grid=(rows // TILE,),
        in_specs=[tiled(TILE, WIDTH)] * 3 + [whole(WIDTH, WIDTH)] * 2,
        out_specs=[tiled(TILE, WIDTH)] * 2,
        out_shape=[jax.ShapeDtypeStruct((rows, WIDTH), F32)] * 2,
        compiler_params=params(8),
        name="finish",
    )(sol, r, image, ah, al)


def exchange(value):
    return lax.all_to_all(value, WIDE_BLK, split_axis=0, concat_axis=0, tiled=True)


def sides(first, last):
    count = lax.axis_size(BLK)
    up = [(i, (i + 1) % count) for i in range(count)]
    down = [(j, i) for i, j in up]
    return lax.ppermute(last, BLK, up), lax.ppermute(first, BLK, down)


def shards(rhs, near_blocks, source_basis, target_basis, far_coupling, send_ids, far_list):
    leaves = rhs.shape[0] // LEAF
    ids = send_ids.reshape(-1)
    readers = far_list.reshape(-1)
    source = source_basis.T
    incoming = exchange(front(ids, rhs, source))
    coup = far_coupling.transpose(0, 2, 1, 3).reshape(leaves * RANK, 4 * RANK)
    left = near_blocks[:NEAR, :HALO]
    right = near_blocks[-NEAR:, -HALO:]
    lo, hi = sides(rhs[:HALO], rhs[-HALO:])
    base0, err = near0(rhs, near_blocks, source)
    image0, first0, last0, trans0, gp0, outgoing = far0(
        ids, readers, incoming, coup, target_basis, source, base0, rhs, err, lo, hi, left, right
    )
    total = summed(exchange(gp0))
    total, outgoing = lax.optimization_barrier((total, outgoing))
    whole0 = exchange(total)
    incoming1 = exchange(outgoing)
    ilo, ihi = sides(first0, last0)
    _, ah, al = solve(whole0)
    r1, base1, sol = near1(rhs, image0, ah, al, near_blocks)
    image1, gp1 = far1(
        readers, incoming1, coup, target_basis, base1, r1, trans0, ah, al, lo, hi, ilo, ihi, left, right
    )
    whole1 = exchange(summed(exchange(gp1)))
    _, bh, bl = solve(whole1)
    return tuple(finish(sol, r1, image1, bh, bl))


def solution(mesh):
    split = Mesh(mesh.devices.reshape(4, 2, 4, 4), ("wide_0", "wide_1", "blk_0", "blk_1"))
    return jax.shard_map(
        shards,
        mesh=split,
        in_specs=(
            P(WIDE_BLK, None),
            P(WIDE_BLK, None),
            P(WIDE_BLK, None),
            P(WIDE_BLK, None),
            P(WIDE_BLK, None, None, None),
            P(WIDE_BLK, None, None),
            P(WIDE_BLK, None),
        ),
        out_specs=(P(WIDE_BLK, None), P(WIDE_BLK, None)),
        check_vma=False,
    )
```

```python
import jax
import jax.numpy as jnp
from jax import lax
from jax.experimental import pallas as pl
from jax.experimental.pallas import tpu as pltpu
from jax.sharding import Mesh
from jax.sharding import PartitionSpec as P

NEAR = 1024
HALO = 256
LEAF = 128
RANK = 64
WIDTH = 256
TILE = 512
FULL = 56
BLK = ("blk_0", "blk_1")
WIDE_BLK = ("wide_0", "wide_1", "blk_0", "blk_1")
F32 = jnp.float32
BF16 = jnp.bfloat16
HIGHEST = lax.Precision.HIGHEST


def params(mib):
    return pltpu.CompilerParams(
        dimension_semantics=("arbitrary",), vmem_limit_bytes=mib * 1024 * 1024
    )


def whole(*shape):
    return pl.BlockSpec(shape, lambda t: (0,) * len(shape), pipeline_mode=pl.Buffered(1))


def kept(*shape):
    return pl.BlockSpec(shape, lambda t: (0,) * len(shape))


def tiled(*shape):
    return pl.BlockSpec(shape, lambda t: (t,) + (0,) * (len(shape) - 1))


def across(rows, cols):
    return pl.BlockSpec((rows, cols), lambda t: (0, t))


def smem():
    return pl.BlockSpec(memory_space=pltpu.SMEM)


def hbm():
    return pl.BlockSpec(memory_space=pltpu.HBM)


def dot(a, b):
    return jnp.dot(a, b, preferred_element_type=F32)


def dot_t(a, b):
    return lax.dot_general(a, b, (((0,), (0,)), ((), ())), preferred_element_type=F32)


def halves(x):
    hi = x.astype(BF16)
    return hi, (x - hi.astype(F32)).astype(BF16)


def dot3(x, hi, lo):
    xh, xl = halves(x)
    return dot(xh, hi) + (dot(xl, hi) + dot(xh, lo))


def send_rows(packed, ids, out, sem, count):
    def one(d, carry):
        pltpu.make_async_copy(packed.at[ids[d]], out.at[d], sem).start()
        return carry

    lax.fori_loop(0, count, one, 0, unroll=8)
    pltpu.make_async_copy(out, out, sem).wait()


def front_kernel(ids, r, s, out, packed, sem):
    t = pl.program_id(0)
    vb = r[...].astype(BF16)
    per = TILE // LEAF
    for i in range(per):
        rows = slice(i * LEAF, (i + 1) * LEAF)
        packed[t * per + i] = dot(s[:, rows], vb[rows]).astype(BF16)

    @pl.when(t == pl.num_programs(0) - 1)
    def _():
        send_rows(packed, ids, out, sem, out.shape[0])


def front(ids, r, s):
    rows = r.shape[0]
    count = ids.shape[0]
    return pl.pallas_call(
        front_kernel,
        grid=(rows // TILE,),
        in_specs=[smem(), tiled(TILE, WIDTH), across(RANK, TILE)],
        out_specs=hbm(),
        out_shape=pltpu.HBM((count, RANK, WIDTH), BF16),
        scratch_shapes=[
            pltpu.VMEM((rows // LEAF, RANK, WIDTH), BF16),
            pltpu.SemaphoreType.DMA(()),
        ],
        compiler_params=params(FULL),
        name="front",
    )(ids, r, s)


def near0_kernel(r, near, s, base, err, ext):
    t = pl.program_id(0)
    rows = r.shape[0]

    @pl.when(t == 0)
    def _():
        ext[:HALO] = jnp.zeros((HALO, WIDTH), BF16)
        ext[HALO : HALO + rows] = r[...].astype(BF16)
        ext[HALO + rows :] = jnp.zeros((HALO, WIDTH), BF16)

    first = pl.multiple_of((t // (NEAR // TILE)) * NEAR, NEAR)
    own = r[pl.ds(pl.multiple_of(t * TILE, TILE), TILE)]
    base[...] = own + dot(near[...], ext[pl.ds(first, NEAR + 2 * HALO)])
    rh, rl = halves(own)
    for i in range(TILE // LEAF):
        cut = slice(i * LEAF, (i + 1) * LEAF)
        high = dot(s[:, cut], rh[cut])
        low = dot(s[:, cut], rl[cut])
        err[i] = (high.astype(BF16).astype(F32) - high) - low


def near0(r, near, s):
    rows = r.shape[0]
    per = TILE // LEAF
    return pl.pallas_call(
        near0_kernel,
        grid=(rows // TILE,),
        in_specs=[
            whole(rows, WIDTH),
            tiled(TILE, NEAR + 2 * HALO),
            across(RANK, TILE),
        ],
        out_specs=[tiled(TILE, WIDTH), tiled(per, RANK, WIDTH)],
        out_shape=[
            jax.ShapeDtypeStruct((rows, WIDTH), F32),
            jax.ShapeDtypeStruct((rows // LEAF, RANK, WIDTH), F32),
        ],
        scratch_shapes=[pltpu.VMEM((rows + 2 * HALO, WIDTH), BF16)],
        compiler_params=params(FULL),
        cost_estimate=pl.CostEstimate(flops=4_000_000_000, bytes_accessed=24_000_000, transcendentals=0),
        name="near0",
    )(r, near, s)


def gram_step(t, image, r, acc):
    ih, il = halves(image)
    rh, rl = halves(r)

    @pl.when(t == 0)
    def _():
        acc[...] = jnp.zeros(acc.shape, F32)

    high = jnp.concatenate([ih.T, rh.T], axis=0)
    low = jnp.concatenate([il.T, rl.T], axis=0)
    acc[...] += dot(jnp.concatenate([high, high, low], axis=1), jnp.concatenate([ih, il, ih], axis=0))
    return ih, il


def gram_end(acc, out):
    for i in range(2 * WIDTH // 8):
        for h in range(2):
            out[2 * i + h] = acc[8 * i : 8 * i + 8, 128 * h : 128 * h + 128]


def fetch_slots(t, readers, incoming, slots, sems):
    count = 4 * (TILE // LEAF)

    def start(step):
        for k in range(count):
            pltpu.make_async_copy(
                incoming.at[readers[step * count + k]],
                slots.at[step % 2, pl.ds(k * RANK, RANK)],
                sems.at[step % 2],
            ).start()

    @pl.when(t == 0)
    def _():
        start(t)

    @pl.when(t + 1 < pl.num_programs(0))
    def _():
        start(t + 1)

    now = slots.at[t % 2]
    pltpu.make_async_copy(now, now, sems.at[t % 2]).wait()
    return now


def edge_specs(tiles):
    edge = NEAR // TILE
    return [
        whole(HALO, WIDTH),
        whole(HALO, WIDTH),
        pl.BlockSpec((TILE, HALO), lambda t: (jnp.minimum(t, edge - 1), 0)),
        pl.BlockSpec((TILE, HALO), lambda t: (jnp.maximum(t - (tiles - edge), 0), 0)),
    ]


def add_edges(t, image, first, last, left, right):
    edge = NEAR // TILE

    @pl.when(t < edge)
    def _():
        image[...] += dot(left[...], first())

    @pl.when(t >= pl.num_programs(0) - edge)
    def _():
        image[...] += dot(right[...], last())


def far0_kernel(ids, readers, incoming, coup, tb, s, base, r, err, lo, hi, left, right, image, first, last, trans, gp, out, packed, direct, saved, acc, slots, sems, sem):
    t = pl.program_id(0)
    per = TILE // LEAF
    now = fetch_slots(t, readers, incoming, slots, sems)
    tiles = []
    for i in range(per):
        cut = slice(i * LEAF, (i + 1) * LEAF)
        tr = dot(coup[i * RANK : (i + 1) * RANK], now[4 * i * RANK : 4 * (i + 1) * RANK])
        trans[i * RANK : (i + 1) * RANK] = tr
        tiles.append(base[cut] + dot(tb[cut], tr.astype(BF16)))
    image[...] = jnp.concatenate(tiles, axis=0)
    add_edges(t, image, lambda: lo[...].astype(BF16), lambda: hi[...].astype(BF16), left, right)

    @pl.when(t == 0)
    def _():
        first[...] = image[:HALO]

    @pl.when(t == pl.num_programs(0) - 1)
    def _():
        last[...] = image[TILE - HALO :]

    ih, il = gram_step(t, image[...], r[...], acc)
    for i in range(per):
        cut = slice(i * LEAF, (i + 1) * LEAF)
        direct[t * per + i] = dot(s[:, cut], ih[cut]) + dot(s[:, cut], il[cut])
        saved[t * per + i] = err[i]

    @pl.when(t == pl.num_programs(0) - 1)
    def _():
        gram_end(acc, gp)
        gram, total = acc[:WIDTH], acc[WIDTH:]
        eye = lax.broadcasted_iota(jnp.int32, gram.shape, 0) == lax.broadcasted_iota(jnp.int32, gram.shape, 1)
        g = jnp.sum(jnp.where(eye, gram, 0.0), axis=0, keepdims=True)
        p = jnp.sum(jnp.where(eye, total, 0.0), axis=0, keepdims=True)
        fits = (4.0 * p > g) & (4.0 * g > p)
        guess = jnp.where(fits, g / jnp.where(fits, p, 1.0), 0.0)
        for leaf in range(packed.shape[0]):
            packed[leaf] = (direct[leaf] + saved[leaf] * guess).astype(BF16)
        send_rows(packed, ids, out, sem, out.shape[0])


def far0(ids, readers, incoming, coup, tb, s, base, r, err, lo, hi, left, right):
    rows = r.shape[0]
    leaves = rows // LEAF
    count = ids.shape[0]
    per = TILE // LEAF
    return pl.pallas_call(
        far0_kernel,
        grid=(rows // TILE,),
        in_specs=[
            smem(),
            smem(),
            hbm(),
            tiled(per * RANK, 4 * RANK),
            tiled(TILE, RANK),
            across(RANK, TILE),
            tiled(TILE, WIDTH),
            tiled(TILE, WIDTH),
            tiled(per, RANK, WIDTH),
            *edge_specs(rows // TILE),
        ],
        out_specs=[
            tiled(TILE, WIDTH),
            kept(HALO, WIDTH),
            kept(HALO, WIDTH),
            tiled(per * RANK, WIDTH),
            kept(128, 8, 128),
            hbm(),
        ],
        out_shape=[
            jax.ShapeDtypeStruct((rows, WIDTH), F32),
            jax.ShapeDtypeStruct((HALO, WIDTH), F32),
            jax.ShapeDtypeStruct((HALO, WIDTH), F32),
            jax.ShapeDtypeStruct((leaves * RANK, WIDTH), F32),
            jax.ShapeDtypeStruct((128, 8, 128), F32),
            pltpu.HBM((count, RANK, WIDTH), BF16),
        ],
        scratch_shapes=[
            pltpu.VMEM((leaves, RANK, WIDTH), BF16),
            pltpu.VMEM((leaves, RANK, WIDTH), F32),
            pltpu.VMEM((leaves, RANK, WIDTH), F32),
            pltpu.VMEM((2 * WIDTH, WIDTH), F32),
            pltpu.VMEM((2, 4 * per * RANK, WIDTH), BF16),
            pltpu.SemaphoreType.DMA((2,)),
            pltpu.SemaphoreType.DMA(()),
        ],
        compiler_params=params(FULL),
        name="far0",
    )(ids, readers, incoming, coup, tb, s, base, r, err, lo, hi, left, right)


def sum_kernel(parts, out):
    total = jnp.sum(parts[...], axis=0)
    out[...] = jnp.broadcast_to(total[None], out.shape)


def summed(parts):
    return pl.pallas_call(
        sum_kernel,
        out_shape=jax.ShapeDtypeStruct(parts.shape, F32),
        compiler_params=pltpu.CompilerParams(vmem_limit_bytes=8 * 1024 * 1024),
        name="summed",
    )(parts)


def lane(x, c):
    return jnp.broadcast_to(x[:, c : c + 1], (8, 128))


def sub(x, k):
    return jnp.broadcast_to(x[k : k + 1, :], (8, 128))


def inverse(rows):
    lanes = lax.broadcasted_iota(jnp.int32, (8, 128), 1)
    subs = lax.broadcasted_iota(jnp.int32, (8, 128), 0)
    rows = list(rows)
    count = len(rows)
    for p in range(count):
        pivot = rows[p]
        cols = [lane(pivot, 8 * p + j) for j in range(8)]
        for k in range(8):
            inv = 1.0 / sub(cols[k], k)
            ck = cols[k]
            here = subs == k
            scaled = sub(pivot, k) * inv
            pivot = jnp.where(here, scaled, pivot - ck * scaled)
            for j in range(8):
                if j != k:
                    cj = sub(cols[j], k) * inv
                    cols[j] = jnp.where(here, cj, cols[j] - ck * cj)
            cols[k] = jnp.where(here, inv, -ck * inv)
            pivot = jnp.where(lanes == 8 * p + k, cols[k], pivot)
        spread = [sub(pivot, j) for j in range(8)]
        panel = (lanes >= 8 * p) & (lanes < 8 * p + 8)
        for i in range(count):
            if i != p:
                value = jnp.where(panel, 0.0, rows[i])
                for j in range(8):
                    value = value - lane(rows[i], 8 * p + j) * spread[j]
                rows[i] = value
        rows[p] = pivot
    return rows


def exact(a, b):
    return jnp.dot(a, b, preferred_element_type=F32, precision=HIGHEST)


def solve_kernel(gp, alpha, high, low):
    def block(first, i0, i1, h):
        return jnp.concatenate([gp[first + 2 * i + h] for i in range(i0, i1)], axis=0)

    x11 = jnp.concatenate(inverse([gp[2 * i] for i in range(16)]), axis=0)
    a12 = block(0, 0, 16, 1)
    a21 = block(0, 16, 32, 0)
    w = exact(x11, a12)
    b1 = block(64, 0, 32, 0).T
    b2 = block(64, 0, 32, 1).T
    schur = block(0, 16, 32, 1) - exact(a21, w)
    y1 = exact(x11, b1)
    z = b2 - exact(a21, y1)
    x22 = jnp.concatenate(inverse([schur[8 * i : 8 * i + 8] for i in range(16)]), axis=0)
    lower = exact(x22, z)
    upper = y1 - exact(w, lower)
    value = jnp.concatenate([upper, lower], axis=0)
    alpha[...] = value
    hi, lo = halves(value)
    high[...] = hi
    low[...] = lo


def solve(gp):
    return pl.pallas_call(
        solve_kernel,
        out_shape=[
            jax.ShapeDtypeStruct((WIDTH, WIDTH), F32),
            jax.ShapeDtypeStruct((WIDTH, WIDTH), BF16),
            jax.ShapeDtypeStruct((WIDTH, WIDTH), BF16),
        ],
        compiler_params=pltpu.CompilerParams(vmem_limit_bytes=16 * 1024 * 1024),
        cost_estimate=pl.CostEstimate(flops=12_000_000_000, bytes_accessed=1_000_000, transcendentals=0),
        name="solve",
    )(gp)


def near1_kernel(r, image, ah, al, near, resid, base, sol, ext, full):
    t = pl.program_id(0)
    rows = r.shape[0]
    high, low = ah[...], al[...]

    @pl.when(t == 0)
    def _():
        ext[:HALO] = jnp.zeros((HALO, WIDTH), BF16)
        for c in range(rows // TILE):
            cut = slice(c * TILE, (c + 1) * TILE)
            value = r[cut] - dot3(image[cut], high, low)
            full[cut] = value
            ext[HALO + c * TILE : HALO + (c + 1) * TILE] = value.astype(BF16)
        ext[HALO + rows :] = jnp.zeros((HALO, WIDTH), BF16)

    first = pl.multiple_of((t // (NEAR // TILE)) * NEAR, NEAR)
    here = pl.ds(pl.multiple_of(t * TILE, TILE), TILE)
    own = full[here]
    resid[...] = own
    base[...] = own + dot(near[...], ext[pl.ds(first, NEAR + 2 * HALO)])
    sol[...] = dot3(r[here], high, low)


def near1(r, image, ah, al, near):
    rows = r.shape[0]
    return pl.pallas_call(
        near1_kernel,
        grid=(rows // TILE,),
        in_specs=[
            whole(rows, WIDTH),
            whole(rows, WIDTH),
            whole(WIDTH, WIDTH),
            whole(WIDTH, WIDTH),
            tiled(TILE, NEAR + 2 * HALO),
        ],
        out_specs=[tiled(TILE, WIDTH)] * 3,
        out_shape=[jax.ShapeDtypeStruct((rows, WIDTH), F32)] * 3,
        scratch_shapes=[
            pltpu.VMEM((rows + 2 * HALO, WIDTH), BF16),
            pltpu.VMEM((rows, WIDTH), F32),
        ],
        compiler_params=params(FULL),
        cost_estimate=pl.CostEstimate(flops=8_000_000_000, bytes_accessed=36_000_000, transcendentals=0),
        name="near1",
    )(r, image, ah, al, near)


def far1_kernel(readers, incoming, coup, tb, base, r, trans, ah, al, lo, hi, ilo, ihi, left, right, image, gp, acc, slots, sems):
    t = pl.program_id(0)
    per = TILE // LEAF
    now = fetch_slots(t, readers, incoming, slots, sems)
    moved = jnp.concatenate(
        [
            dot(coup[i * RANK : (i + 1) * RANK], now[4 * i * RANK : 4 * (i + 1) * RANK])
            for i in range(per)
        ],
        axis=0,
    )
    tr = (trans[...] - dot3(moved, ah[...], al[...])).astype(BF16)
    tiles = []
    for i in range(per):
        cut = slice(i * LEAF, (i + 1) * LEAF)
        tiles.append(base[cut] + dot(tb[cut], tr[i * RANK : (i + 1) * RANK]))
    image[...] = jnp.concatenate(tiles, axis=0)
    add_edges(
        t,
        image,
        lambda: (lo[...] - dot3(ilo[...], ah[...], al[...])).astype(BF16),
        lambda: (hi[...] - dot3(ihi[...], ah[...], al[...])).astype(BF16),
        left,
        right,
    )
    gram_step(t, image[...], r[...], acc)

    @pl.when(t == pl.num_programs(0) - 1)
    def _():
        gram_end(acc, gp)


def far1(readers, incoming, coup, tb, base, r, trans, ah, al, lo, hi, ilo, ihi, left, right):
    rows = r.shape[0]
    per = TILE // LEAF
    return pl.pallas_call(
        far1_kernel,
        grid=(rows // TILE,),
        in_specs=[
            smem(),
            hbm(),
            tiled(per * RANK, 4 * RANK),
            tiled(TILE, RANK),
            tiled(TILE, WIDTH),
            tiled(TILE, WIDTH),
            tiled(per * RANK, WIDTH),
            whole(WIDTH, WIDTH),
            whole(WIDTH, WIDTH),
            whole(HALO, WIDTH),
            whole(HALO, WIDTH),
            *edge_specs(rows // TILE),
        ],
        out_specs=[tiled(TILE, WIDTH), kept(128, 8, 128)],
        out_shape=[
            jax.ShapeDtypeStruct((rows, WIDTH), F32),
            jax.ShapeDtypeStruct((128, 8, 128), F32),
        ],
        scratch_shapes=[
            pltpu.VMEM((2 * WIDTH, WIDTH), F32),
            pltpu.VMEM((2, 4 * per * RANK, WIDTH), BF16),
            pltpu.SemaphoreType.DMA((2,)),
        ],
        compiler_params=params(FULL),
        name="far1",
    )(readers, incoming, coup, tb, base, r, trans, ah, al, lo, hi, ilo, ihi, left, right)


def finish_kernel(sol, r, image, ah, al, solution, residual):
    high, low = ah[...], al[...]
    solution[...] = sol[...] + dot3(r[...], high, low)
    residual[...] = r[...] - dot3(image[...], high, low)


def finish(sol, r, image, ah, al):
    rows = r.shape[0]
    return pl.pallas_call(
        finish_kernel,
        grid=(rows // TILE,),
        in_specs=[tiled(TILE, WIDTH)] * 3 + [whole(WIDTH, WIDTH)] * 2,
        out_specs=[tiled(TILE, WIDTH)] * 2,
        out_shape=[jax.ShapeDtypeStruct((rows, WIDTH), F32)] * 2,
        compiler_params=params(8),
        name="finish",
    )(sol, r, image, ah, al)


def exchange(value):
    return lax.all_to_all(value, WIDE_BLK, split_axis=0, concat_axis=0, tiled=True)


def sides(first, last):
    count = lax.axis_size(BLK)
    up = [(i, (i + 1) % count) for i in range(count)]
    down = [(j, i) for i, j in up]
    return lax.ppermute(last, BLK, up), lax.ppermute(first, BLK, down)


def shards(rhs, near_blocks, source_basis, target_basis, far_coupling, send_ids, far_list):
    leaves = rhs.shape[0] // LEAF
    ids = send_ids.reshape(-1)
    readers = far_list.reshape(-1)
    source = source_basis.T
    incoming = exchange(front(ids, rhs, source))
    coup = far_coupling.transpose(0, 2, 1, 3).reshape(leaves * RANK, 4 * RANK)
    left = near_blocks[:NEAR, :HALO]
    right = near_blocks[-NEAR:, -HALO:]
    lo, hi = sides(rhs[:HALO], rhs[-HALO:])
    base0, err = near0(rhs, near_blocks, source)
    image0, first0, last0, trans0, gp0, outgoing = far0(
        ids, readers, incoming, coup, target_basis, source, base0, rhs, err, lo, hi, left, right
    )
    total = summed(exchange(gp0))
    total, outgoing = lax.optimization_barrier((total, outgoing))
    whole0 = exchange(total)
    incoming1 = exchange(outgoing)
    ilo, ihi = sides(first0, last0)
    _, ah, al = solve(whole0)
    r1, base1, sol = near1(rhs, image0, ah, al, near_blocks)
    image1, gp1 = far1(
        readers, incoming1, coup, target_basis, base1, r1, trans0, ah, al, lo, hi, ilo, ihi, left, right
    )
    whole1 = exchange(summed(exchange(gp1)))
    _, bh, bl = solve(whole1)
    return tuple(finish(sol, r1, image1, bh, bl))


def solution(mesh):
    split = Mesh(mesh.devices.reshape(4, 2, 4, 4), ("wide_0", "wide_1", "blk_0", "blk_1"))
    return jax.shard_map(
        shards,
        mesh=split,
        in_specs=(
            P(WIDE_BLK, None),
            P(WIDE_BLK, None),
            P(WIDE_BLK, None),
            P(WIDE_BLK, None),
            P(WIDE_BLK, None, None, None),
            P(WIDE_BLK, None, None),
            P(WIDE_BLK, None),
        ),
        out_specs=(P(WIDE_BLK, None), P(WIDE_BLK, None)),
        check_vma=False,
    )
```
